256 devices in a mesh: subj: 16 (over y_hi, z), slab: 16 (over x, y_lo, core).
Axes of the slice: x: 4, y: 4 (y_hi: 2, y_lo: 2; y = y_hi * 2 + y_lo), z: 8, core: 2. Of those that a mesh axis runs over, the one named last changes fastest.
Arguments:
- fod: bfloat16 [64, 45, 8192], P('subj', None, 'slab'), may hold values from -24 to 24
- rotation: bfloat16 [64, 45, 45, 8192], P('subj', None, None, 'slab'), may hold values from -0.875 to 0.875
- modulation: float32 [64, 8192], P('subj', 'slab'), may hold values from 0.3 to 3
- subject_ids: int32 [64], P('subj'), may hold values from 0 to 63, each once
- subject_weight: float32 [64], replicated, may hold values from 0.5 to 2
- voxel_cell_index: int32 [8192], P('slab'), may hold values from 0 to 1023, as said below
Outputs:
- template: bfloat16 [45, 16384], replicated
The draws below stay inside these ranges and needn't reach their ends.
Inputs may be any that keep to these rules, and one draw needn't show every extreme that they name: `voxel_cell_index`: within each aligned block of 512 entries (one slab's masked voxels) the cell numbers are distinct and increasing.
All inputs are finite; a program needn't handle non-finite values.
Results may differ from the reference program's by a relative error of at most 0.001.
Values may be sent and summed in bfloat16 or wider, within the bound.
A program may use at most 64 MiB of HBM per device.

```python
import math
import jax
import jax.numpy as jnp
from jax import lax

COEF = 45
VOX_DEV = 512
GRID_DEV = 1024
SUBJECTS = 64
MASKED_VOXELS = 8192
N_SLAB = 16


def draw_voxel_cell_index(key, part):
    keys = jax.random.split(jax.random.fold_in(key, 7), N_SLAB)

    def single_slab_block(slab_key):
        order = jax.random.permutation(slab_key, GRID_DEV)
        return jnp.sort(order[:VOX_DEV])
    blocks = jax.vmap(single_slab_block)(keys)
    return blocks.reshape(VOX_DEV * N_SLAB).astype(jnp.int32)


def block_scale(own_key, dims, shards, low, high):
    loudness = 1.0
    for dim, blocks in shards:
        draws = jax.random.uniform(jax.random.fold_in(jax.random.fold_in(own_key, 6), dim), (blocks,), jnp.float32, low / len(shards), high / len(shards))
        loudness = loudness * jnp.repeat(jnp.exp(draws), dims[dim] // blocks).reshape((-1,) + (1,) * (len(dims) - 1 - dim))
    return loudness


def bell_draw(rng, extent, width, bound, shards=(), kind=jnp.bfloat16):
    factor_of = block_scale(rng, extent, shards, -0.22, 0.18) if shards else 1.0
    values = jax.random.normal(rng, extent, jnp.float32) * width * factor_of
    return jnp.minimum(jnp.maximum(values, -bound), bound).astype(kind)


def setup_inputs(seed: int = 0) -> dict:
    seeds = jax.random.split(jax.random.key(seed), 7)
    fod = bell_draw(seeds[0], (SUBJECTS, COEF, MASKED_VOXELS), 4.0, 24.0, ((0, 16), (2, 16)))
    rotation = bell_draw(seeds[1], (SUBJECTS, COEF, COEF, MASKED_VOXELS), COEF ** -0.5, 0.875, ((0, 16), (3, 16)))
    modulation = jnp.clip(jnp.exp(math.log(3.0) - 2.3025851 * jax.random.uniform(seeds[2], (SUBJECTS, MASKED_VOXELS), jnp.float32) ** block_scale(seeds[2], (SUBJECTS, MASKED_VOXELS), ((0, 16), (1, 16)), -0.2, 0.2)), 0.3, 3.0)
    subject_ids = jax.random.permutation(seeds[3], SUBJECTS).astype(jnp.int32)
    subject_weight = jnp.clip(jnp.exp(jax.random.uniform(seeds[4], (SUBJECTS,), jnp.float32, math.log(0.5), math.log(2.0))), 0.5, 2.0)
    voxel_cell_index = draw_voxel_cell_index(jax.random.fold_in(seeds[6], 71), 0)
    return {"fod": fod, "rotation": rotation, "modulation": modulation, "subject_ids": subject_ids, "subject_weight": subject_weight, "voxel_cell_index": voxel_cell_index}


def reference(fod, rotation, modulation, subject_ids, subject_weight, voxel_cell_index):
    selected_cells = subject_weight[subject_ids]
    weight = modulation * selected_cells[:, None]

    def accumulate_weighted(total, items):
        rot_one, fod_one, weight_one = items
        rotated_coefficients = jnp.einsum("ckv,kv->cv", rot_one.astype(jnp.float32), fod_one.astype(jnp.float32))
        return total + rotated_coefficients * weight_one[None, :], None

    start = jnp.zeros((COEF, MASKED_VOXELS), jnp.float32)
    numer, unused = lax.scan(accumulate_weighted, start, (rotation, fod, weight))
    denom = jnp.sum(weight, axis=0)
    average = (numer / denom[None, :]).astype(jnp.bfloat16)
    slab_lookup = (jnp.arange(MASKED_VOXELS, dtype=jnp.int32) // VOX_DEV).astype(jnp.int32)
    cells = (voxel_cell_index + slab_lookup * GRID_DEV).astype(jnp.int32)
    template = jnp.zeros((COEF, GRID_DEV * N_SLAB), jnp.bfloat16)
    return template.at[:, cells].set(average)
```

```python
import functools
import jax
import jax.numpy as jnp
from jax import lax
from jax.experimental import pallas as pl
from jax.experimental.pallas import tpu as pltpu
from jax.sharding import PartitionSpec as P

COEF = 45
SUBJ_DEV = 4
LANES = 128
QUARTERS = 4
BLOCKS = 8
GROUPS = 3
OWNERS = GROUPS * QUARTERS
CHUNK = 8
MESH = pl.DeviceIdType.MESH


def cell_map(cells):
    voxels = cells.shape[1]
    high = cells // LANES
    low = cells - high * LANES
    row = lax.broadcasted_iota(jnp.int32, (BLOCKS, voxels), 0)
    lane = lax.broadcasted_iota(jnp.int32, (LANES, voxels), 0)
    one, zero = jnp.float32(1), jnp.float32(0)
    here = jnp.where(high == row, one, zero)
    before = jnp.where(high < row, one, zero)
    less = jnp.where(low < lane, one, zero)
    same = jnp.where(low == lane, one, zero)
    nt = (((1,), (1,)), ((), ()))
    bf = jnp.bfloat16
    rank = lax.dot_general(here.astype(bf), less.astype(bf), nt, preferred_element_type=jnp.float32)
    mask = lax.dot_general(here.astype(bf), same.astype(bf), nt, preferred_element_type=jnp.float32)
    rank = rank + jnp.sum(before, axis=1, keepdims=True)
    return jnp.where(mask > 0.5, rank, -1.0).astype(jnp.int32)


def kernel(n_subj, n_slab, rot_hbm, fod_hbm, mod_hbm, cells_hbm, ids_ref, sw_ref, out_ref,
           rot, fod_b, fod, mod, cells, prod, sums, got, den, slabs, maps,
           rot_sem, in_sem, rs_send, rs_recv, dn_send, dn_recv, ag_send, ag_recv,
           sl_send, sl_recv, sib_send, sib_recv, mp_send, mp_recv):
    me = lax.axis_index("subj")
    slab = lax.axis_index("slab")
    sib = slab + 1 - 2 * lax.rem(slab, 2)
    core = lax.rem(slab, 2)

    ins = [
        pltpu.make_async_copy(mod_hbm, mod, in_sem.at[0]),
        pltpu.make_async_copy(fod_hbm, fod_b, in_sem.at[1]),
        pltpu.make_async_copy(cells_hbm, cells, in_sem.at[2]),
    ]
    for c in ins:
        c.start()
    chunks = []
    for i, c0 in enumerate(range(0, COEF, CHUNK)):
        n = min(CHUNK, COEF - c0)
        cp = pltpu.make_async_copy(rot_hbm.at[pl.ds(c0, n)], rot.at[pl.ds(c0, n)], rot_sem.at[i])
        cp.start()
        chunks.append((c0, n, cp))

    barrier = pltpu.get_barrier_semaphore()

    def greet(k, _):
        pl.semaphore_signal(barrier, inc=1, device_id=(lax.rem(me + k, n_subj), slab), device_id_type=MESH)
        return 0

    lax.fori_loop(1, n_subj, greet, 0)

    def greet_slab(k, _):
        pl.semaphore_signal(barrier, inc=1, device_id=(me, lax.rem(slab + k, n_slab)), device_id_type=MESH)
        return 0

    lax.fori_loop(1, n_slab, greet_slab, 0)

    ins[0].wait()
    row = lax.rem(lax.broadcasted_iota(jnp.int32, (16, LANES), 0), SUBJ_DEV)
    scale = jnp.full((16, LANES), sw_ref[ids_ref[0]], jnp.float32)
    for s in range(1, SUBJ_DEV):
        scale = jnp.where(row == s, sw_ref[ids_ref[s]], scale)
    mod[...] = mod[...] * scale
    parts = [mod[pl.ds(s, QUARTERS, stride=SUBJ_DEV), :] for s in range(SUBJ_DEV)]
    den[me] = (parts[0] + parts[1]) + (parts[2] + parts[3])

    ins[2].wait()
    maps[slab] = cell_map(cells[...])

    ins[1].wait()
    fod[...] = fod_b[...].astype(jnp.float32)

    def compute(c0, n):
        def step(k, acc):
            f = fod[k]
            return tuple(acc[i] + rot[c0 + i, k].astype(jnp.float32) * f for i in range(n))

        acc = lax.fori_loop(0, COEF, step, tuple(jnp.zeros((16, LANES), jnp.float32) for _ in range(n)), unroll=9)
        w = mod[...]
        for i in range(n):
            y = acc[i] * w
            prod[0, pl.ds((c0 + i) * 8, 8), :] = y[:8]
            prod[1, pl.ds((c0 + i) * 8, 8), :] = y[8:]

    def gather_group(g):
        for t in range(QUARTERS):
            for h in range(2):
                base = (16 * g + 8 * h) * 8 + 4 * (t % 2)
                p = [prod[t // 2, pl.ds(base + s, 8, stride=8), :] for s in range(SUBJ_DEV)]
                sums[4 * g + t, pl.ds(8 * h, 8), :] = (p[0] + p[1]) + (p[2] + p[3])

    def rs_copy(owner, src):
        return pltpu.make_async_remote_copy(
            src_ref=sums.at[owner], dst_ref=got.at[src], send_sem=rs_send.at[owner],
            recv_sem=rs_recv.at[src], device_id=(owner, slab), device_id_type=MESH)

    def dn_copy(owner, src):
        return pltpu.make_async_remote_copy(
            src_ref=den.at[me], dst_ref=den.at[src], send_sem=dn_send.at[owner],
            recv_sem=dn_recv.at[src], device_id=(owner, slab), device_id_type=MESH)

    def send_group(g):
        def one(t, _):
            owner = 4 * g + lax.rem(t + me, 4)

            @pl.when(owner != me)
            def _():
                rs_copy(owner, me).start()

            return 0

        lax.fori_loop(0, QUARTERS, one, 0)

    prod[:, COEF * 8:, :] = jnp.zeros((2, 3 * 8, LANES), jnp.float32)

    def map_copy(k):
        peer = lax.rem(slab + k, n_slab)
        return pltpu.make_async_remote_copy(
            src_ref=maps.at[slab], dst_ref=maps.at[slab], send_sem=mp_send.at[k],
            recv_sem=mp_recv.at[slab], device_id=(me, peer), device_id_type=MESH)

    def map_wait(src):
        return pltpu.make_async_remote_copy(
            src_ref=maps.at[src], dst_ref=maps.at[src], send_sem=mp_send.at[0],
            recv_sem=mp_recv.at[src], device_id=(me, sib), device_id_type=MESH)

    for i, (c0, n, cp) in enumerate(chunks):
        cp.wait()
        compute(c0, n)
        if i == 1:
            gather_group(0)
            pl.semaphore_wait(barrier, n_subj - 1 + n_slab - 1)

            def send_dn(k, _):
                owner = lax.rem(me + k, n_subj)

                @pl.when(owner < OWNERS)
                def _():
                    dn_copy(owner, me).start()

                return 0

            lax.fori_loop(1, n_subj, send_dn, 0)
            send_group(0)

            def send_map(k, _):
                map_copy(k).start()
                return 0

            lax.fori_loop(1, n_slab, send_map, 0)
        if i == 3:
            gather_group(1)
            send_group(1)
    gather_group(2)
    send_group(2)

    def tile_copy(dst):
        return pltpu.make_async_remote_copy(
            src_ref=slabs.at[slab, me], dst_ref=slabs.at[slab, me], send_sem=ag_send.at[dst],
            recv_sem=ag_recv.at[me], device_id=(dst, slab), device_id_type=MESH)

    def tile_wait(owner):
        return pltpu.make_async_remote_copy(
            src_ref=slabs.at[slab, owner], dst_ref=slabs.at[slab, owner], send_sem=ag_send.at[owner],
            recv_sem=ag_recv.at[owner], device_id=(owner, slab), device_id_type=MESH)

    @pl.when(me < OWNERS)
    def _():
        t = lax.rem(me, QUARTERS)

        def add_den(k, total):
            src = lax.rem(me + k, n_subj)
            dn_copy(0, src).wait_recv()
            return total + den[src]

        total_den = lax.fori_loop(1, n_subj, add_den, den[me])
        quarter = lax.broadcasted_iota(jnp.int32, (QUARTERS, LANES), 0)
        mine = jnp.sum(jnp.where(quarter == t, total_den, 0.0), axis=0, keepdims=True)

        def add(k, total):
            src = lax.rem(me + k, n_subj)
            rs_copy(0, src).wait_recv()
            return total + got[src]

        total = lax.fori_loop(1, n_subj, add, sums[me])
        slabs[slab, me] = (total / mine).astype(jnp.bfloat16)

        def send(k, _):
            tile_copy(lax.rem(me + k, n_subj)).start()
            return 0

        lax.fori_loop(1, n_subj, send, 0)

    def await_tile(k, _):
        owner = lax.rem(me + k, n_subj)

        @pl.when(owner < OWNERS)
        def _():
            tile_wait(owner).wait_recv()

        return 0

    lax.fori_loop(1, n_subj, await_tile, 0)

    chips = n_slab // 2

    def slab_copy(q, dst, send_sem, recv_sem):
        return pltpu.make_async_remote_copy(
            src_ref=slabs.at[q], dst_ref=slabs.at[q], send_sem=send_sem, recv_sem=recv_sem,
            device_id=(me, dst), device_id_type=MESH)

    def partner(k):
        return lax.rem(slab // 2 + k, chips) * 2 + core

    def send_slab(k, _):
        slab_copy(slab, partner(k), sl_send.at[k], sl_recv.at[slab]).start()
        return 0

    lax.fori_loop(1, chips, send_slab, 0)
    slab_copy(slab, sib, sib_send.at[0], sib_recv.at[slab]).start()

    def expand(q):
        base = pl.multiple_of(q * (BLOCKS * LANES), BLOCKS * LANES)
        for b in range(BLOCKS):
            ranks = jnp.broadcast_to(maps[q, pl.ds(b, 1), :], (8, LANES))
            source = ranks // LANES
            lane = ranks - source * LANES
            lane = jnp.where(ranks < 0, 0, lane)
            low, high = max(0, b - 4), min(b, 3)
            for g in range(GROUPS):
                tiles = [slabs[q, 4 * g + t].astype(jnp.float32) for t in range(low, high + 1)]
                halves = []
                for h in range(2):
                    value = jnp.zeros((8, LANES), jnp.float32)
                    for t, tile in zip(range(low, high + 1), tiles):
                        picked = jnp.take_along_axis(tile[8 * h:8 * h + 8], lane, axis=1)
                        value = jnp.where((ranks >= 0) & (source == t), picked, value)
                    halves.append(value)
                both = jnp.concatenate(halves, axis=0).astype(jnp.bfloat16)
                rows = min(16, COEF - 16 * g)
                out_ref[pl.ds(16 * g, rows), pl.ds(pl.multiple_of(base + b * LANES, LANES), LANES)] = both[:rows]

    def await_maps(k, _):
        map_wait(lax.rem(slab + k, n_slab)).wait_recv()
        return 0

    lax.fori_loop(1, n_slab, await_maps, 0)

    def visit(k, _):
        @pl.when((k > 0) & (k < chips))
        def _():
            q = partner(chips - k)
            slab_copy(q, sib, sl_send.at[0], sl_recv.at[q]).wait_recv()
            slab_copy(q, sib, sib_send.at[k], sib_recv.at[q]).start()

        @pl.when(k >= chips)
        def _():
            q = lax.rem(sib // 2 + 2 * chips - k, chips) * 2 + lax.rem(sib, 2)
            slab_copy(q, sib, sib_send.at[0], sib_recv.at[q]).wait_recv()

        q = lax.rem(slab // 2 + 2 * chips - k, chips) * 2 + jnp.where(k < chips, core, 1 - core)
        expand(q)
        return 0

    lax.fori_loop(0, 2 * chips, visit, 0)

    def drain_slab(k, _):
        slab_copy(slab, partner(k), sl_send.at[k], sl_recv.at[slab]).wait_send()
        return 0

    lax.fori_loop(1, chips, drain_slab, 0)

    def drain_sib(k, _):
        slab_copy(slab, sib, sib_send.at[k], sib_recv.at[slab]).wait_send()
        return 0

    lax.fori_loop(0, chips, drain_sib, 0)

    def drain_map(k, _):
        map_copy(k).wait_send()
        return 0

    lax.fori_loop(1, n_slab, drain_map, 0)

    def drain_subj(k, _):
        peer = lax.rem(me + k, n_subj)

        @pl.when(peer < OWNERS)
        def _():
            rs_copy(peer, me).wait_send()
            dn_copy(peer, me).wait_send()

        @pl.when(me < OWNERS)
        def _():
            tile_copy(peer).wait_send()

        return 0

    lax.fori_loop(1, n_subj, drain_subj, 0)


def on_device(n_subj, n_slab, fod, rotation, modulation, subject_ids, subject_weight, voxel_cell_index):
    rot = rotation.reshape(SUBJ_DEV, COEF, COEF, QUARTERS, LANES).transpose(1, 2, 3, 0, 4).reshape(COEF, COEF, 16, LANES)
    fo = fod.reshape(SUBJ_DEV, COEF, QUARTERS, LANES).transpose(1, 2, 0, 3).reshape(COEF, 16, LANES)
    mod = modulation.reshape(SUBJ_DEV, QUARTERS, LANES).transpose(1, 0, 2).reshape(16, LANES)
    cells = voxel_cell_index.reshape(1, QUARTERS * LANES)
    n_chunks = -(-COEF // CHUNK)
    dma = pltpu.SemaphoreType.DMA
    hbm = pl.BlockSpec(memory_space=pltpu.HBM)
    smem = pl.BlockSpec(memory_space=pltpu.SMEM)
    chips = n_slab // 2
    return pl.pallas_call(
        functools.partial(kernel, n_subj, n_slab),
        out_shape=jax.ShapeDtypeStruct((COEF, n_slab * BLOCKS * LANES), jnp.bfloat16),
        in_specs=[hbm, hbm, hbm, hbm, smem, smem],
        out_specs=pl.BlockSpec(memory_space=pltpu.VMEM),
        scratch_shapes=[
            pltpu.VMEM((COEF, COEF, 16, LANES), jnp.bfloat16),
            pltpu.VMEM((COEF, 16, LANES), jnp.bfloat16),
            pltpu.VMEM((COEF, 16, LANES), jnp.float32),
            pltpu.VMEM((16, LANES), jnp.float32),
            pltpu.VMEM((1, QUARTERS * LANES), jnp.int32),
            pltpu.VMEM((2, 48 * 8, LANES), jnp.float32),
            pltpu.VMEM((OWNERS, 16, LANES), jnp.float32),
            pltpu.VMEM((n_subj, 16, LANES), jnp.float32),
            pltpu.VMEM((n_subj, QUARTERS, LANES), jnp.float32),
            pltpu.VMEM((n_slab, OWNERS, 16, LANES), jnp.bfloat16),
            pltpu.VMEM((n_slab, BLOCKS, LANES), jnp.int32),
            dma((n_chunks,)), dma((3,)),
            dma((n_subj,)), dma((n_subj,)), dma((n_subj,)), dma((n_subj,)),
            dma((n_subj,)), dma((n_subj,)),
            dma((chips,)), dma((n_slab,)), dma((chips,)), dma((n_slab,)),
            dma((n_slab,)), dma((n_slab,)),
        ],
        compiler_params=pltpu.CompilerParams(
            collective_id=0, has_side_effects=True, vmem_limit_bytes=60 * 1024 * 1024),
    )(rot, fo, mod, cells, subject_ids, subject_weight)


def solution(mesh):
    placed = (
        P("subj", None, "slab"),
        P("subj", None, None, "slab"),
        P("subj", "slab"),
        P("subj"),
        P(),
        P("slab"),
    )
    body = functools.partial(on_device, mesh.shape["subj"], mesh.shape["slab"])
    return jax.shard_map(body, mesh=mesh, in_specs=placed, out_specs=P(), check_vma=False)
```
